128 devices in a mesh: row: 8 (over y, x_hi), col: 16 (over x_lo, z, core).
Axes of the slice: x: 4 (x_hi: 2, x_lo: 2; x = x_hi * 2 + x_lo), y: 4, z: 4, core: 2. Of those that a mesh axis runs over, the one named last changes fastest.
Arguments:
- left_matrix: float32 [4096, 4096], P('row', 'col'), may hold values from -6 to 6
- right_matrix: float32 [4096, 4096], P('row', 'col'), may hold values from -0.09375 to 0.09375
Outputs:
- product_matrix: float32 [4096, 4096], P('row', 'col')
The draws below stay inside these ranges and needn't reach their ends.
All inputs are finite; a program needn't handle non-finite values.
Results may differ from the reference program's by a relative error of at most 0.00019.
Values sent between devices are 32-bit elements; how exact they have to be, the bound alone decides.
No kernel may reach another device: no remote copies, remote signals or barrier semaphores. Data moves between devices by JAX's collectives and lax.ppermute only.
A program may use at most 64 MiB of HBM per device.

```python
import jax
import jax.numpy as jnp
from jax import lax

ORDER = 4096


def level_of(own_key, dims, split, least, high):
    def one(position, blocks):
        steps = jax.random.uniform(jax.random.fold_in(jax.random.fold_in(own_key, 6), position), (blocks,), jnp.float32, least / len(split), high / len(split))
        return jnp.repeat(jnp.exp(steps), dims[position] // blocks).reshape((-1,) + (1,) * (len(dims) - position - 1))

    gain = one(*split[0])
    for cut in split[1:]:
        gain = gain * one(*cut)
    return gain


def scatter_about(own_key, extent, spread, reach, split=(), dtype=jnp.bfloat16):
    gain = level_of(own_key, extent, split, -0.22, 0.18) if split else 1.0
    result = jax.random.normal(own_key, extent, jnp.float32) * spread * gain
    return jnp.minimum(jnp.maximum(result, -reach), reach).astype(dtype)


def setup_inputs(seed: int = 0) -> dict:
    arg_keys = jax.random.split(jax.random.key(seed), 3)
    left_matrix = scatter_about(arg_keys[0], (ORDER, ORDER), 1.0, 6.0, ((0, 8), (1, 16)), jnp.float32)
    right_matrix = scatter_about(arg_keys[1], (ORDER, ORDER), ORDER ** -0.5, 0.09375, ((0, 8), (1, 16)), jnp.float32)
    return {"left_matrix": left_matrix, "right_matrix": right_matrix}


def multiply(left_term, right_term):
    return jnp.dot(left_term, right_term, precision=lax.Precision.HIGHEST, preferred_element_type=jnp.float32)


def left_terms(upper_left, upper_right, lower_left, lower_right):
    sum_one = lower_left + lower_right
    sum_two = sum_one - upper_left
    sum_three = upper_left - lower_left
    sum_four = upper_right - sum_two
    return (upper_left, upper_right, sum_four, lower_right, sum_one, sum_two, sum_three)


def right_terms(upper_left, upper_right, lower_left, lower_right):
    diff_one = upper_right - upper_left
    diff_two = lower_right - diff_one
    diff_three = lower_right - upper_right
    diff_four = diff_two - lower_left
    return (upper_left, lower_left, lower_right, diff_four, diff_one, diff_two, diff_three)


def reference(left_matrix, right_matrix):
    half_order = ORDER // 2
    lefts = left_terms(left_matrix[:half_order, :half_order], left_matrix[:half_order, half_order:],
                       left_matrix[half_order:, :half_order], left_matrix[half_order:, half_order:])
    rights = right_terms(right_matrix[:half_order, :half_order], right_matrix[:half_order, half_order:],
                         right_matrix[half_order:, :half_order], right_matrix[half_order:, half_order:])
    products = [multiply(lefts[index], rights[index]) for index in range(7)]
    partial_two = products[0] + products[5]
    partial_three = partial_two + products[6]
    partial_four = partial_two + products[4]
    upper_left = products[0] + products[1]
    upper_right = partial_four + products[2]
    lower_left = partial_three - products[3]
    lower_right = partial_three + products[4]
    return jnp.block([[upper_left, upper_right], [lower_left, lower_right]])
```

```python
import jax
import jax.numpy as jnp
from jax import lax
from jax.experimental import pallas as pl
from jax.experimental.pallas import tpu as pltpu
from jax.sharding import PartitionSpec as P


BOTH = ("row", "col")
Y, XH, XL, Z, CORE = 4, 2, 2, 4, 2
F32, BF16 = jnp.float32, jnp.bfloat16


def pairs(move):
    listed = []
    for y in range(Y):
        for x in range(XH * XL):
            for z in range(Z):
                for core in range(CORE):
                    y2, x2, z2, core2 = move(y, x, z, core)
                    y2, x2, z2 = y2 % Y, x2 % (XH * XL), z2 % Z
                    source = ((y * XH + x // XL) * XL + x % XL) * Z + z
                    target = ((y2 * XH + x2 // XL) * XL + x2 % XL) * Z + z2
                    listed.append((source * CORE + core, target * CORE + core2))
    return listed


MOVES = {
    "z+": pairs(lambda y, x, z, c: (y, x, z + 1, c)),
    "z-": pairs(lambda y, x, z, c: (y, x, z - 1, c)),
    "y+": pairs(lambda y, x, z, c: (y + 1, x, z, c)),
    "y-": pairs(lambda y, x, z, c: (y - 1, x, z, c)),
    "lo": pairs(lambda y, x, z, c: (y, x ^ 1, z, c)),
    "hi": pairs(lambda y, x, z, c: (y, x ^ 2, z, c)),
    "core": pairs(lambda y, x, z, c: (y, x, z, 1 - c)),
}


def send(array, move):
    return lax.ppermute(array, BOTH, MOVES[move])


def cut(array, top, rows):
    return array[top : top + rows]


def place():
    row, col = lax.axis_index("row"), lax.axis_index("col")
    y, xh = row >> 1, row & 1
    xl, z, core = col >> 3, (col >> 1) & 3, col & 1
    left = lambda other, turn: ((xl ^ other) * Z) + ((z + turn) & 3)
    right = lambda other, turn: (((y + turn) & 3) * XH) + (xh ^ other)
    return left, right, core


def split(value):
    high = value.astype(BF16)
    return high, (value - high.astype(F32)).astype(BF16)


def mul(left, high, low):
    left_high, left_low = split(left)
    dot = lambda one, two: jnp.dot(one, two, preferred_element_type=F32)
    return dot(left_high, high) + (dot(left_low, high) + dot(left_high, low))


LEFTS = ((0, 0, 0), (1, 0, 0), (0, 3, 0), (0, 1, 0), (0, 2, 0), (0, 2, 1), (1, 3, 0), (1, 1, 0))
RIGHTS = ((0, 0, 0), (0, 3, 0), (0, 1, 0), (0, 2, 0), (0, 2, 1), (1, 0, 0), (1, 0, 1), (1, 3, 0), (1, 1, 0), (1, 3, 1), (1, 1, 1))


def main_kernel(*refs):
    count = len(LEFTS)
    mine, theirs, rights = refs[:count], refs[count : 2 * count], refs[2 * count : 2 * count + len(RIGHTS)]
    total, held_left, held_high, held_low, high, low = refs[2 * count + len(RIGHTS) :]
    left_of, right_of, core = place()
    last = right_of(1, 2)
    spare = left_of(1, 2)
    step = high.shape[1]

    for ref, (other, turn, half) in zip(rights, RIGHTS):
        for part in range(ref.shape[0] // step):
            at = right_of(other, turn) * 2 + half + part
            high[at], low[at] = split(ref[part * step : (part + 1) * step])
    for part in range(2):
        high[last * 2 + part] = jnp.zeros(high.shape[1:], BF16)
        low[last * 2 + part] = jnp.zeros(low.shape[1:], BF16)
    for part in range(2):
        held_high[part] = high[spare * 2 + part]
        held_low[part] = low[spare * 2 + part]

    begun = False
    for refs, side in ((mine, core), (theirs, 1 - core)):
        for ref, (other, turn, half) in zip(refs, LEFTS):
            tile = left_of(other, turn)
            rows = ref.shape[0]
            at = tile * 2 + side
            top = half * rows
            for block in range(rows // step):
                rows_in = pl.ds(block * step, step)
                rows_out = pl.ds(top + block * step, step)
                product = mul(ref[rows_in], high[at], low[at])
                if begun:
                    total[rows_out] += product
                else:
                    total[rows_out] = product

            begun = True

            @pl.when(tile == last)
            def _():
                held_left[side, pl.ds(top, rows)] = ref[...]


def last_kernel(total, held_left, held_high, held_low, a0, a1, s0, s1, b0, b1, b2, b3, out, high, low):
    left_of, right_of, core = place()
    last = right_of(1, 2)
    spare = left_of(1, 2)
    step = high.shape[1]
    for index, ref in enumerate((b0, b1, b2, b3)):
        rows = ref.shape[0]
        at = pl.ds(index % 2 * rows, rows)
        high[index // 2, at], low[index // 2, at] = split(ref[...])

    @pl.when(last == spare)
    def _():
        held_high[...] = high[...]
        held_low[...] = low[...]

    for block, (mine, theirs) in enumerate(((a0, s0), (a1, s1))):
        rows = pl.ds(block * step, step)
        out[rows] = (
            total[rows]
            + mul(mine[...], held_high[core], held_low[core])
            + mul(theirs[...], held_high[1 - core], held_low[1 - core])
        )

    @pl.when(last != spare)
    def _():
        for block in range(2):
            rows = pl.ds(block * step, step)
            out[rows] += mul(held_left[0, rows], high[0], low[0]) + mul(held_left[1, rows], high[1], low[1])


def product(a, b):
    tall, wide = a.shape
    deep, broad = b.shape
    half, quarter, hill = deep // 2, deep // 4, tall // 2
    inside = pl.BlockSpec(memory_space=pltpu.VMEM)

    a_lo = send(a, "lo")
    a_p, a_m = send(a, "z+"), send(a, "z-")
    b_p, b_m = send(b, "y+"), send(b, "y-")
    b_hi = [send(cut(b, 0, half), "hi"), send(cut(b, half, half), "hi")]
    al_p, al_m = send(a_lo, "z+"), send(a_lo, "z-")
    a_pp = send(cut(a_p, 0, hill), "z+")
    a_mm = send(cut(a_m, hill, hill), "z-")
    b_pp = send(cut(b_p, 0, half), "y+")
    b_mm = send(cut(b_m, half, half), "y-")
    bh_p = [send(b_hi[0], "y+"), send(b_hi[1], "y+")]
    bh_m = [send(b_hi[0], "y-"), send(b_hi[1], "y-")]
    al_pp = send(cut(al_p, 0, hill), "z+")
    al_mm = send(cut(al_m, hill, hill), "z-")
    bh_pp = [send(cut(bh_p[0], 0, quarter), "y+"), send(cut(bh_p[1], 0, quarter), "y+")]
    bh_mm = [send(cut(bh_m[0], quarter, quarter), "y-"), send(cut(bh_m[1], quarter, quarter), "y-")]

    lefts = (a, a_lo, a_p, a_m, a_pp, a_mm, al_p, al_m)
    others = tuple(send(piece, "core") for piece in lefts)
    rights = (b, b_p, b_m, b_pp, b_mm, b_hi[0], b_hi[1], bh_p[0], bh_m[0], bh_p[1], bh_m[1])
    step = half
    flops = 6 * tall * deep * XL * Z * broad
    total, held_left, held_high, held_low = pl.pallas_call(
        main_kernel,
        out_shape=(
            jax.ShapeDtypeStruct((tall, broad), F32),
            jax.ShapeDtypeStruct((2, tall, wide), F32),
            jax.ShapeDtypeStruct((2, step, broad), BF16),
            jax.ShapeDtypeStruct((2, step, broad), BF16),
        ),
        in_specs=[inside] * (2 * len(lefts) + len(rights)),
        out_specs=(inside,) * 4,
        scratch_shapes=[pltpu.VMEM((XL * Z * 2, step, broad), BF16)] * 2,
        compiler_params=pltpu.CompilerParams(vmem_limit_bytes=24 << 20),
        cost_estimate=pl.CostEstimate(flops=flops, bytes_accessed=12 << 20, transcendentals=0),
    )(*lefts, *others, *rights)

    last_s = send(al_pp, "core"), send(al_mm, "core")
    return pl.pallas_call(
        last_kernel,
        out_shape=jax.ShapeDtypeStruct((tall, broad), F32),
        in_specs=[inside] * 12,
        out_specs=inside,
        scratch_shapes=[pltpu.VMEM((2, step, broad), BF16)] * 2,
        compiler_params=pltpu.CompilerParams(vmem_limit_bytes=12 << 20),
        cost_estimate=pl.CostEstimate(flops=flops // 4, bytes_accessed=3 << 20, transcendentals=0),
    )(total, held_left, held_high, held_low, al_pp, al_mm, *last_s, bh_pp[0], bh_mm[0], bh_pp[1], bh_mm[1])


def solution(mesh):
    placed = (P("row", "col"), P("row", "col"))
    return jax.shard_map(product, mesh=mesh, in_specs=placed, out_specs=P("row", "col"), check_vma=False)
```

```python
import jax
import jax.numpy as jnp
from jax import lax
from jax.experimental import pallas as pl
from jax.experimental.pallas import tpu as pltpu
from jax.sharding import PartitionSpec as P


BOTH = ("row", "col")
Y, XH, XL, Z, CORE = 4, 2, 2, 4, 2
F32, BF16 = jnp.float32, jnp.bfloat16


def pairs(move):
    listed = []
    for y in range(Y):
        for x in range(XH * XL):
            for z in range(Z):
                for core in range(CORE):
                    y2, x2, z2, core2 = move(y, x, z, core)
                    y2, x2, z2 = y2 % Y, x2 % (XH * XL), z2 % Z
                    source = ((y * XH + x // XL) * XL + x % XL) * Z + z
                    target = ((y2 * XH + x2 // XL) * XL + x2 % XL) * Z + z2
                    listed.append((source * CORE + core, target * CORE + core2))
    return listed


MOVES = {
    "z+": pairs(lambda y, x, z, c: (y, x, z + 1, 1 - c)),
    "z-": pairs(lambda y, x, z, c: (y, x, z - 1, 1 - c)),
    "y+": pairs(lambda y, x, z, c: (y + 1, x, z, c)),
    "y-": pairs(lambda y, x, z, c: (y - 1, x, z, c)),
    "lo": pairs(lambda y, x, z, c: (y, x ^ 1, z, 1 - c)),
    "hi": pairs(lambda y, x, z, c: (y, x ^ 2, z, c)),
    "core": pairs(lambda y, x, z, c: (y, x, z, 1 - c)),
}


def send(array, move):
    return lax.ppermute(array, BOTH, MOVES[move])


def cut(array, top, rows):
    return array[top : top + rows]


def place():
    row, col = lax.axis_index("row"), lax.axis_index("col")
    y, xh = row >> 1, row & 1
    xl, z, core = col >> 3, (col >> 1) & 3, col & 1
    left = lambda other, turn: ((xl ^ other) * Z) + ((z + turn) & 3)
    right = lambda other, turn: (((y + turn) & 3) * XH) + (xh ^ other)
    return left, right, core


def split(value):
    high = value.astype(BF16)
    return high, (value - high.astype(F32)).astype(BF16)


def mul(*terms):
    lefts, rights = [], []
    for left, high, low in terms:
        left_high, left_low = split(left)
        lefts += [left_high, left_low, left_high]
        rights += [high, high, low]
    return jnp.dot(jnp.concatenate(lefts, axis=1), jnp.concatenate(rights), preferred_element_type=F32)


LEFTS = ((0, 0, 0), (1, 0, 0), (0, 3, 0), (0, 1, 0), (0, 2, 0), (0, 2, 1), (1, 3, 0), (1, 1, 0))
ROWS, FAR = 64, 256
RIGHTS = (
    (0, 0, 0), (0, 3, 0), (0, 1, 0), (0, 2, 0), (0, 2, FAR), (1, 0, 0), (1, 0, 256),
    (1, 3, 0), (1, 1, 0), (1, 3, 256), (1, 1, 256),
)
SOON, HELD = 4, 7


def store_right(refs, places, right_of, high, low):
    step = high.shape[1]
    for ref, (other, turn, top) in zip(refs, places):
        for part in range(0, ref.shape[0], ROWS):
            at, rows = right_of(other, turn) * 2 + (top + part) // step, pl.ds((top + part) % step, ROWS)
            high[at, rows], low[at, rows] = split(ref[part : part + ROWS])


def add(total, mine, theirs, place_of, left_of, core, high, low):
    other, turn, half = place_of
    tile = left_of(other, turn)
    rows, step = mine.shape[0], high.shape[1]
    side = (core + other + turn) & 1
    at, beside = tile * 2 + side, tile * 2 + 1 - side
    for block in range(rows // step):
        rows_in = pl.ds(block * step, step)
        rows_out = pl.ds(half * rows + block * step, step)
        total[rows_out] += mul((mine[rows_in], high[at], low[at]), (theirs[rows_in], high[beside], low[beside]))


def is_soon(tile, right_of):
    return ((tile & 1) == (right_of(0, 0) & 1)) | (tile == right_of(1, 0))


def soon_kernel(*refs):
    mine, theirs, rights = refs[:SOON], refs[SOON : 2 * SOON], refs[2 * SOON : 2 * SOON + HELD]
    total, high, low = refs[2 * SOON + HELD :]
    left_of, right_of, core = place()
    store_right(rights, RIGHTS[:HELD], right_of, high, low)
    total[...] = jnp.zeros_like(total)
    for mine_ref, their_ref, where in zip(mine, theirs, LEFTS):

        @pl.when(is_soon(left_of(*where[:2]), right_of))
        def _():
            add(total, mine_ref, their_ref, where, left_of, core, high, low)


def main_kernel(*refs):
    count, late = len(LEFTS), len(RIGHTS) - HELD
    mine, theirs, rights = refs[:count], refs[count : 2 * count], refs[2 * count : 2 * count + late]
    _, _, _, total, high, low, held_left, held_high, held_low = refs[2 * count + late :]
    left_of, right_of, core = place()
    last = right_of(1, 2)
    spare = left_of(1, 2)

    store_right(rights, RIGHTS[HELD:], right_of, high, low)
    for part in range(2):
        high[last * 2 + part] = jnp.zeros(high.shape[1:], BF16)
        low[last * 2 + part] = jnp.zeros(low.shape[1:], BF16)

    @pl.when(last == spare)
    def _():
        held_left[...] = jnp.zeros_like(held_left)

    for part in range(2):
        held_high[part] = high[spare * 2 + part]
        held_low[part] = low[spare * 2 + part]

    for index, (mine_ref, their_ref, where) in enumerate(zip(mine, theirs, LEFTS)):
        other, turn, half = where
        tile = left_of(other, turn)
        rows = mine_ref.shape[0]
        if index < SOON:

            @pl.when(jnp.logical_not(is_soon(tile, right_of)))
            def _():
                add(total, mine_ref, their_ref, where, left_of, core, high, low)

        else:
            add(total, mine_ref, their_ref, where, left_of, core, high, low)

        @pl.when(tile == last)
        def _():
            side = (core + other + turn) & 1
            held_left[side, pl.ds(half * rows, rows)] = mine_ref[...]
            held_left[1 - side, pl.ds(half * rows, rows)] = their_ref[...]


def last_kernel(total, held_left, held_high, held_low, a0, a1, s0, s1, b0, b1, out, high, low, done, sems):
    left_of, right_of, core = place()
    last = right_of(1, 2)
    spare = left_of(1, 2)
    step = high.shape[1]
    for index, ref in enumerate((b0, b1)):
        high[index], low[index] = split(ref[...])

    @pl.when(last == spare)
    def _():
        held_high[...] = high[...]
        held_low[...] = low[...]

    side = 1 - core
    copies = []
    for block, (mine, theirs) in enumerate(((a0, s0), (a1, s1))):
        rows = pl.ds(block * step, step)
        done[rows] = total[rows] + mul(
            (mine[...], held_high[side], held_low[side]),
            (theirs[...], held_high[1 - side], held_low[1 - side]),
            (held_left[0, rows], high[0], low[0]),
            (held_left[1, rows], high[1], low[1]),
        )
        copies.append(pltpu.make_async_copy(done.at[rows], out.at[rows], sems.at[block]))
        copies[-1].start()
    for copy in copies:
        copy.wait()


def product(a, b):
    tall, wide = a.shape
    deep, broad = b.shape
    half, hill = deep // 2, tall // 2
    inside = pl.BlockSpec(memory_space=pltpu.VMEM)

    a_lo = send(a, "lo")
    a_p, a_m = send(a, "z+"), send(a, "z-")
    b_p, b_m = send(b, "y+"), send(b, "y-")
    b_hi = [send(cut(b, 0, half), "hi"), send(cut(b, half, half), "hi")]
    al_p, al_m = send(a_lo, "z+"), send(a_lo, "z-")
    a_pp = send(cut(a_p, 0, hill), "z+")
    a_mm = send(cut(a_m, hill, hill), "z-")
    b_pp = send(cut(b_p, 0, FAR), "y+")
    b_mm = send(cut(b_m, FAR, deep - FAR), "y-")
    bh_p = [send(b_hi[0], "y+"), send(b_hi[1], "y+")]
    bh_m = [send(b_hi[0], "y-"), send(b_hi[1], "y-")]
    al_pp = send(cut(al_p, 0, hill), "z+")
    al_mm = send(cut(al_m, hill, hill), "z-")
    far_b = send(bh_p[0], "y+"), send(bh_m[1], "y-")

    lefts = (a, a_lo, a_p, a_m, a_pp, a_mm, al_p, al_m)
    others = tuple(send(piece, "core") for piece in lefts)
    rights = (b, b_p, b_m, b_pp, b_mm, b_hi[0], b_hi[1], bh_p[0], bh_m[0], bh_p[1], bh_m[1])
    step = half
    flops = 6 * tall * deep * XL * Z * broad
    shape = jax.ShapeDtypeStruct
    whole, panel = shape((tall, broad), F32), shape((XL * Z * 2, step, broad), BF16)

    def cost(part):
        return pl.CostEstimate(flops=flops * part // 8, bytes_accessed=part << 20, transcendentals=0)

    soon = (*lefts[:SOON], *others[:SOON], *rights[:HELD])
    total, high, low = pl.pallas_call(
        soon_kernel,
        out_shape=(whole, panel, panel),
        in_specs=[inside] * len(soon),
        out_specs=(inside,) * 3,
        compiler_params=pltpu.CompilerParams(vmem_limit_bytes=16 << 20),
        cost_estimate=cost(2),
    )(*soon)
    later = (*lefts, *others, *rights[HELD:])
    total, _, _, held_left, held_high, held_low = pl.pallas_call(
        main_kernel,
        out_shape=(
            whole, panel, panel,
            shape((2, tall, wide), F32),
            shape((2, step, broad), BF16),
            shape((2, step, broad), BF16),
        ),
        in_specs=[inside] * (len(later) + 3),
        out_specs=(inside,) * 6,
        input_output_aliases={len(later) + index: index for index in range(3)},
        compiler_params=pltpu.CompilerParams(vmem_limit_bytes=16 << 20),
        cost_estimate=cost(5),
    )(*later, total, high, low)

    last_s = send(al_pp, "core"), send(al_mm, "core")
    return pl.pallas_call(
        last_kernel,
        out_shape=jax.ShapeDtypeStruct((tall, broad), F32),
        in_specs=[inside] * 10,
        out_specs=pl.BlockSpec(memory_space=pl.ANY),
        scratch_shapes=[pltpu.VMEM((2, step, broad), BF16)] * 2
        + [pltpu.VMEM((tall, broad), F32), pltpu.SemaphoreType.DMA((2,))],
        compiler_params=pltpu.CompilerParams(vmem_limit_bytes=12 << 20),
        cost_estimate=cost(2),
    )(total, held_left, held_high, held_low, al_pp, al_mm, *last_s, *far_b)


def solution(mesh):
    placed = (P("row", "col"), P("row", "col"))
    return jax.shard_map(product, mesh=mesh, in_specs=placed, out_specs=P("row", "col"), check_vma=False)
```

```python
import jax
import jax.numpy as jnp
from jax import lax
from jax.experimental import pallas as pl
from jax.experimental.pallas import tpu as pltpu
from jax.sharding import PartitionSpec as P


BOTH = ("row", "col")
Y, XH, XL, Z, CORE = 4, 2, 2, 4, 2
F32, BF16 = jnp.float32, jnp.bfloat16


def pairs(move):
    listed = []
    for y in range(Y):
        for x in range(XH * XL):
            for z in range(Z):
                for core in range(CORE):
                    y2, x2, z2, core2 = move(y, x, z, core)
                    y2, x2, z2 = y2 % Y, x2 % (XH * XL), z2 % Z
                    source = ((y * XH + x // XL) * XL + x % XL) * Z + z
                    target = ((y2 * XH + x2 // XL) * XL + x2 % XL) * Z + z2
                    listed.append((source * CORE + core, target * CORE + core2))
    return listed


MOVES = {
    "z+": pairs(lambda y, x, z, c: (y, x, z + 1, 1 - c)),
    "z-": pairs(lambda y, x, z, c: (y, x, z - 1, 1 - c)),
    "y+": pairs(lambda y, x, z, c: (y + 1, x, z, c)),
    "y-": pairs(lambda y, x, z, c: (y - 1, x, z, c)),
    "lo": pairs(lambda y, x, z, c: (y, x ^ 1, z, 1 - c)),
    "hi": pairs(lambda y, x, z, c: (y, x ^ 2, z, c)),
    "core": pairs(lambda y, x, z, c: (y, x, z, 1 - c)),
}


def send(array, move):
    return lax.ppermute(array, BOTH, MOVES[move])


def cut(array, top, rows):
    return array[top : top + rows]


def place():
    row, col = lax.axis_index("row"), lax.axis_index("col")
    y, xh = row >> 1, row & 1
    xl, z, core = col >> 3, (col >> 1) & 3, col & 1
    left = lambda other, turn: ((xl ^ other) * Z) + ((z + turn) & 3)
    right = lambda other, turn: (((y + turn) & 3) * XH) + (xh ^ other)
    return left, right, core


def split(value):
    high = value.astype(BF16)
    return high, (value - high.astype(F32)).astype(BF16)


def mul(*terms):
    lefts, rights = [], []
    for left, high, low in terms:
        left_high, left_low = split(left)
        lefts += [left_high, left_low, left_high]
        rights += [high, high, low]
    return jnp.dot(jnp.concatenate(lefts, axis=1), jnp.concatenate(rights), preferred_element_type=F32)


LEFTS = ((0, 0, 0), (1, 0, 0), (0, 3, 0), (0, 1, 0), (0, 2, 0), (0, 2, 1), (1, 3, 0), (1, 1, 0))
ROWS, FAR = 64, 256
RIGHTS = (
    (0, 0, 0), (0, 3, 0), (0, 1, 0), (0, 2, 0), (0, 2, FAR), (1, 0, 0), (1, 0, 256),
    (1, 3, 0), (1, 1, 0), (1, 3, 256), (1, 1, 256),
)
SOON, HELD = 4, 7


def store_right(refs, places, right_of, high, low):
    step = high.shape[1]
    for ref, (other, turn, top) in zip(refs, places):
        for part in range(0, ref.shape[0], ROWS):
            at, rows = right_of(other, turn) * 2 + (top + part) // step, pl.ds((top + part) % step, ROWS)
            high[at, rows], low[at, rows] = split(ref[part : part + ROWS])


def add(total, mine, theirs, place_of, left_of, core, high, low):
    other, turn, half = place_of
    tile = left_of(other, turn)
    rows, step = mine.shape[0], high.shape[1]
    side = (core + other + turn) & 1
    at, beside = tile * 2 + side, tile * 2 + 1 - side
    for block in range(rows // step):
        rows_in = pl.ds(block * step, step)
        rows_out = pl.ds(half * rows + block * step, step)
        total[rows_out] += mul((mine[rows_in], high[at], low[at]), (theirs[rows_in], high[beside], low[beside]))


def is_soon(tile, right_of):
    return ((tile & 1) == (right_of(0, 0) & 1)) | (tile == right_of(1, 0))


def soon_kernel(*refs):
    mine, theirs, rights = refs[:SOON], refs[SOON : 2 * SOON], refs[2 * SOON : 2 * SOON + HELD]
    total, high, low = refs[2 * SOON + HELD :]
    left_of, right_of, core = place()
    store_right(rights, RIGHTS[:HELD], right_of, high, low)
    total[...] = jnp.zeros_like(total)
    for mine_ref, their_ref, where in zip(mine, theirs, LEFTS):

        @pl.when(is_soon(left_of(*where[:2]), right_of))
        def _():
            add(total, mine_ref, their_ref, where, left_of, core, high, low)


def main_kernel(*refs):
    count, late = len(LEFTS), len(RIGHTS) - HELD
    mine, theirs, rights = refs[:count], refs[count : 2 * count], refs[2 * count : 2 * count + late]
    _, _, _, total, high, low, held_left, held_high, held_low = refs[2 * count + late :]
    left_of, right_of, core = place()
    last = right_of(1, 2)
    spare = left_of(1, 2)

    store_right(rights, RIGHTS[HELD:], right_of, high, low)
    for part in range(2):
        high[last * 2 + part] = jnp.zeros(high.shape[1:], BF16)
        low[last * 2 + part] = jnp.zeros(low.shape[1:], BF16)

    @pl.when(last == spare)
    def _():
        held_left[...] = jnp.zeros_like(held_left)

    for part in range(2):
        held_high[part] = high[spare * 2 + part]
        held_low[part] = low[spare * 2 + part]

    for index, (mine_ref, their_ref, where) in enumerate(zip(mine, theirs, LEFTS)):
        other, turn, half = where
        tile = left_of(other, turn)
        rows = mine_ref.shape[0]
        open_still = tile != last
        if index < SOON:
            open_still &= jnp.logical_not(is_soon(tile, right_of))

        @pl.when(open_still)
        def _():
            add(total, mine_ref, their_ref, where, left_of, core, high, low)

        @pl.when(tile == last)
        def _():
            side = (core + other + turn) & 1
            held_left[side, pl.ds(half * rows, rows)] = mine_ref[...]
            held_left[1 - side, pl.ds(half * rows, rows)] = their_ref[...]


def last_kernel(total, held_left, held_high, held_low, a0, a1, s0, s1, b0, b1, out, high, low, done, sems):
    left_of, right_of, core = place()
    last = right_of(1, 2)
    spare = left_of(1, 2)
    step = high.shape[1]
    for index, ref in enumerate((b0, b1)):
        high[index], low[index] = split(ref[...])

    @pl.when(last == spare)
    def _():
        held_high[...] = high[...]
        held_low[...] = low[...]

    side = 1 - core
    copies = []
    for block, (mine, theirs) in enumerate(((a0, s0), (a1, s1))):
        rows = pl.ds(block * step, step)
        done[rows] = total[rows] + mul(
            (mine[...], held_high[side], held_low[side]),
            (theirs[...], held_high[1 - side], held_low[1 - side]),
            (held_left[0, rows], high[0], low[0]),
            (held_left[1, rows], high[1], low[1]),
        )
        copies.append(pltpu.make_async_copy(done.at[rows], out.at[rows], sems.at[block]))
        copies[-1].start()
    for copy in copies:
        copy.wait()


def product(a, b):
    tall, wide = a.shape
    deep, broad = b.shape
    half, hill = deep // 2, tall // 2
    inside = pl.BlockSpec(memory_space=pltpu.VMEM)

    a_lo = send(a, "lo")
    a_p, a_m = send(a, "z+"), send(a, "z-")
    b_p, b_m = send(b, "y+"), send(b, "y-")
    b_hi = [send(cut(b, 0, half), "hi"), send(cut(b, half, half), "hi")]
    al_p, al_m = send(a_lo, "z+"), send(a_lo, "z-")
    a_pp = send(cut(a_p, 0, hill), "z+")
    a_mm = send(cut(a_m, hill, hill), "z-")
    b_pp = send(cut(b_p, 0, FAR), "y+")
    b_mm = send(cut(b_m, FAR, deep - FAR), "y-")
    bh_p = [send(b_hi[0], "y+"), send(b_hi[1], "y+")]
    bh_m = [send(b_hi[0], "y-"), send(b_hi[1], "y-")]
    al_pp = send(cut(al_p, 0, hill), "z+")
    al_mm = send(cut(al_m, hill, hill), "z-")
    far_b = send(bh_p[0], "y+"), send(bh_m[1], "y-")

    lefts = (a, a_lo, a_p, a_m, a_pp, a_mm, al_p, al_m)
    others = tuple(send(piece, "core") for piece in lefts)
    rights = (b, b_p, b_m, b_pp, b_mm, b_hi[0], b_hi[1], bh_p[0], bh_m[0], bh_p[1], bh_m[1])
    step = half
    flops = 6 * tall * deep * XL * Z * broad
    shape = jax.ShapeDtypeStruct
    whole, panel = shape((tall, broad), F32), shape((XL * Z * 2, step, broad), BF16)

    def cost(part):
        return pl.CostEstimate(flops=flops * part // 8, bytes_accessed=part << 20, transcendentals=0)

    soon = (*lefts[:SOON], *others[:SOON], *rights[:HELD])
    total, high, low = pl.pallas_call(
        soon_kernel,
        out_shape=(whole, panel, panel),
        in_specs=[inside] * len(soon),
        out_specs=(inside,) * 3,
        compiler_params=pltpu.CompilerParams(vmem_limit_bytes=16 << 20),
        cost_estimate=cost(2),
    )(*soon)
    later = (*lefts, *others, *rights[HELD:])
    total, _, _, held_left, held_high, held_low = pl.pallas_call(
        main_kernel,
        out_shape=(
            whole, panel, panel,
            shape((2, tall, wide), F32),
            shape((2, step, broad), BF16),
            shape((2, step, broad), BF16),
        ),
        in_specs=[inside] * (len(later) + 3),
        out_specs=(inside,) * 6,
        input_output_aliases={len(later) + index: index for index in range(3)},
        compiler_params=pltpu.CompilerParams(vmem_limit_bytes=16 << 20),
        cost_estimate=cost(5),
    )(*later, total, high, low)

    last_s = send(al_pp, "core"), send(al_mm, "core")
    return pl.pallas_call(
        last_kernel,
        out_shape=jax.ShapeDtypeStruct((tall, broad), F32),
        in_specs=[inside] * 10,
        out_specs=pl.BlockSpec(memory_space=pl.ANY),
        scratch_shapes=[pltpu.VMEM((2, step, broad), BF16)] * 2
        + [pltpu.VMEM((tall, broad), F32), pltpu.SemaphoreType.DMA((2,))],
        compiler_params=pltpu.CompilerParams(vmem_limit_bytes=12 << 20),
        cost_estimate=cost(2),
    )(total, held_left, held_high, held_low, al_pp, al_mm, *last_s, *far_b)


def solution(mesh):
    placed = (P("row", "col"), P("row", "col"))
    return jax.shard_map(product, mesh=mesh, in_specs=placed, out_specs=P("row", "col"), check_vma=False)
```

```python
import jax
import jax.numpy as jnp
from jax import lax
from jax.experimental import pallas as pl
from jax.experimental.pallas import tpu as pltpu
from jax.sharding import PartitionSpec as P


BOTH = ("row", "col")
Y, XH, XL, Z, CORE = 4, 2, 2, 4, 2
F32, BF16 = jnp.float32, jnp.bfloat16


def pairs(move):
    listed = []
    for y in range(Y):
        for x in range(XH * XL):
            for z in range(Z):
                for core in range(CORE):
                    y2, x2, z2, core2 = move(y, x, z, core)
                    y2, x2, z2 = y2 % Y, x2 % (XH * XL), z2 % Z
                    source = ((y * XH + x // XL) * XL + x % XL) * Z + z
                    target = ((y2 * XH + x2 // XL) * XL + x2 % XL) * Z + z2
                    listed.append((source * CORE + core, target * CORE + core2))
    return listed


MOVES = {
    "z+": pairs(lambda y, x, z, c: (y, x, z + 1, 1 - c)),
    "z-": pairs(lambda y, x, z, c: (y, x, z - 1, 1 - c)),
    "y+": pairs(lambda y, x, z, c: (y + 1, x, z, c)),
    "y-": pairs(lambda y, x, z, c: (y - 1, x, z, c)),
    "lo": pairs(lambda y, x, z, c: (y, x ^ 1, z, 1 - c)),
    "hi": pairs(lambda y, x, z, c: (y, x ^ 2, z, c)),
    "core": pairs(lambda y, x, z, c: (y, x, z, 1 - c)),
}


def send(array, move):
    return lax.ppermute(array, BOTH, MOVES[move])


def cut(array, top, rows):
    return array[top : top + rows]


def cat(*arrays):
    return jnp.concatenate(arrays)


def place():
    row, col = lax.axis_index("row"), lax.axis_index("col")
    y, xh = row >> 1, row & 1
    xl, z, core = col >> 3, (col >> 1) & 3, col & 1
    left = lambda other, turn: ((xl ^ other) * Z) + ((z + turn) & 3)
    right = lambda other, turn: (((y + turn) & 3) * XH) + (xh ^ other)
    return left, right, core


def split(value):
    high = value.astype(BF16)
    return high, (value - high.astype(F32)).astype(BF16)


def mul(*terms):
    lefts, rights = [], []
    for left, high, low in terms:
        left_high, left_low = split(left)
        lefts += [left_high, left_low, left_high]
        rights += [high, high, low]
    return jnp.dot(jnp.concatenate(lefts, axis=1), jnp.concatenate(rights), preferred_element_type=F32)


LEFTS = ((0, 0), (1, 0), (0, 3), (0, 1), (0, 2), (1, 3), (1, 1))
ROWS, FAR = 64, 256
RIGHTS = (
    (0, 0, 0), (0, 3, 0), (0, 1, 0), (0, 2, 0), (0, 2, FAR), (1, 0, 0), (1, 0, 256),
    (1, 3, 0), (1, 1, 0), (1, 3, 256), (1, 1, 256),
)
SOON, HELD = 4, 7


def store_right(refs, places, right_of, high, low):
    step = high.shape[1]
    for ref, (other, turn, top) in zip(refs, places):
        for part in range(0, ref.shape[0], ROWS):
            at, rows = right_of(other, turn) * 2 + (top + part) // step, pl.ds((top + part) % step, ROWS)
            high[at, rows], low[at, rows] = split(ref[part : part + ROWS])


def add(total, mine, theirs, place_of, left_of, core, high, low):
    other, turn = place_of
    tile = left_of(other, turn)
    rows, step = mine.shape[0], high.shape[1]
    side = (core + other + turn) & 1
    at, beside = tile * 2 + side, tile * 2 + 1 - side
    for block in range(rows // step):
        rows_in = pl.ds(block * step, step)
        total[rows_in] += mul((mine[rows_in], high[at], low[at]), (theirs[rows_in], high[beside], low[beside]))


def is_soon(tile, right_of):
    return ((tile & 1) == (right_of(0, 0) & 1)) | (tile == right_of(1, 0))


def parts(ref, count):
    rows = ref.shape[0] // count
    return tuple(ref.at[pl.ds(index * rows, rows)] for index in range(count))


def soon_kernel(*refs):
    mine, rights = refs[:SOON], refs[SOON + 2 : SOON + 2 + HELD]
    theirs = (refs[SOON], *parts(refs[SOON + 1], SOON - 1))
    total, high, low = refs[SOON + 2 + HELD :]
    left_of, right_of, core = place()
    store_right(rights, RIGHTS[:HELD], right_of, high, low)
    total[...] = jnp.zeros_like(total)
    for mine_ref, their_ref, where in zip(mine, theirs, LEFTS):

        @pl.when(is_soon(left_of(*where), right_of))
        def _():
            add(total, mine_ref, their_ref, where, left_of, core, high, low)


def main_kernel(*refs):
    count, late = len(LEFTS), len(RIGHTS) - HELD
    mine, rights = refs[:count], refs[count + 4 : count + 4 + late]
    own, one, far, two = refs[count : count + 4]
    theirs = (own, *parts(one, SOON - 1), far, *parts(two, 2))
    _, _, _, total, high, low, held_left, held_high, held_low = refs[count + 4 + late :]
    left_of, right_of, core = place()
    last = right_of(1, 2)
    spare = left_of(1, 2)

    store_right(rights, RIGHTS[HELD:], right_of, high, low)
    for part in range(2):
        high[last * 2 + part] = jnp.zeros(high.shape[1:], BF16)
        low[last * 2 + part] = jnp.zeros(low.shape[1:], BF16)

    @pl.when(last == spare)
    def _():
        held_left[...] = jnp.zeros_like(held_left)

    for part in range(2):
        held_high[part] = high[spare * 2 + part]
        held_low[part] = low[spare * 2 + part]

    for index, (mine_ref, their_ref, where) in enumerate(zip(mine, theirs, LEFTS)):
        other, turn = where
        tile = left_of(other, turn)
        open_still = tile != last
        if index < SOON:
            open_still &= jnp.logical_not(is_soon(tile, right_of))

        @pl.when(open_still)
        def _():
            add(total, mine_ref, their_ref, where, left_of, core, high, low)

        @pl.when(tile == last)
        def _():
            side = (core + other + turn) & 1
            held_left[side] = mine_ref[...]
            held_left[1 - side] = their_ref[...]


def last_kernel(total, held_left, held_high, held_low, mine, theirs, b0, b1, out, high, low, done, sems):
    left_of, right_of, core = place()
    last = right_of(1, 2)
    spare = left_of(1, 2)
    step = high.shape[1]
    for index, ref in enumerate((b0, b1)):
        high[index], low[index] = split(ref[...])

    @pl.when(last == spare)
    def _():
        held_high[...] = high[...]
        held_low[...] = low[...]

    side = 1 - core
    copies = []
    for block in range(mine.shape[0] // step):
        rows = pl.ds(block * step, step)
        done[rows] = total[rows] + mul(
            (mine[rows], held_high[side], held_low[side]),
            (theirs[rows], held_high[1 - side], held_low[1 - side]),
            (held_left[0, rows], high[0], low[0]),
            (held_left[1, rows], high[1], low[1]),
        )
        copies.append(pltpu.make_async_copy(done.at[rows], out.at[rows], sems.at[block]))
        copies[-1].start()
    for copy in copies:
        copy.wait()


def product(a, b):
    tall, wide = a.shape
    deep, broad = b.shape
    half, hill = deep // 2, tall // 2
    inside = pl.BlockSpec(memory_space=pltpu.VMEM)

    a_lo = send(a, "lo")
    a_p, a_m = send(a, "z+"), send(a, "z-")
    b_p, b_m = send(b, "y+"), send(b, "y-")
    b_hi = [send(cut(b, 0, half), "hi"), send(cut(b, half, half), "hi")]
    al_p, al_m = send(a_lo, "z+"), send(a_lo, "z-")
    a_pp = send(cut(a_p, 0, hill), "z+")
    a_mm = send(cut(a_m, hill, hill), "z-")
    b_pp = send(cut(b_p, 0, FAR), "y+")
    b_mm = send(cut(b_m, FAR, deep - FAR), "y-")
    bh_p = [send(b_hi[0], "y+"), send(b_hi[1], "y+")]
    bh_m = [send(b_hi[0], "y-"), send(b_hi[1], "y-")]
    al_pp = send(cut(al_p, 0, hill), "z+")
    al_mm = send(cut(al_m, hill, hill), "z-")
    far_b = send(bh_p[0], "y+"), send(bh_m[1], "y-")

    a_far = cat(a_pp, a_mm)
    lefts = (a, a_lo, a_p, a_m, a_far, al_p, al_m)
    own = send(a, "core")
    one = send(cat(a_lo, a_p, a_m), "core")
    two = send(cat(al_p, al_m), "core")
    far = send(a_far, "core")
    rights = (b, b_p, b_m, b_pp, b_mm, b_hi[0], b_hi[1], bh_p[0], bh_m[0], bh_p[1], bh_m[1])
    step = half
    flops = 6 * tall * deep * XL * Z * broad
    shape = jax.ShapeDtypeStruct
    whole, panel = shape((tall, broad), F32), shape((XL * Z * 2, step, broad), BF16)

    def cost(part):
        return pl.CostEstimate(flops=flops * part // 8, bytes_accessed=part << 20, transcendentals=0)

    soon = (*lefts[:SOON], own, one, *rights[:HELD])
    total, high, low = pl.pallas_call(
        soon_kernel,
        out_shape=(whole, panel, panel),
        in_specs=[inside] * len(soon),
        out_specs=(inside,) * 3,
        compiler_params=pltpu.CompilerParams(vmem_limit_bytes=16 << 20),
        cost_estimate=cost(2),
    )(*soon)
    later = (*lefts, own, one, far, two, *rights[HELD:])
    total, _, _, held_left, held_high, held_low = pl.pallas_call(
        main_kernel,
        out_shape=(
            whole, panel, panel,
            shape((2, tall, wide), F32),
            shape((2, step, broad), BF16),
            shape((2, step, broad), BF16),
        ),
        in_specs=[inside] * (len(later) + 3),
        out_specs=(inside,) * 6,
        input_output_aliases={len(later) + index: index for index in range(3)},
        compiler_params=pltpu.CompilerParams(vmem_limit_bytes=16 << 20),
        cost_estimate=cost(5),
    )(*later, total, high, low)

    last_a = cat(al_pp, al_mm)
    last_s = send(last_a, "core")
    return pl.pallas_call(
        last_kernel,
        out_shape=jax.ShapeDtypeStruct((tall, broad), F32),
        in_specs=[inside] * 8,
        out_specs=pl.BlockSpec(memory_space=pl.ANY),
        scratch_shapes=[pltpu.VMEM((2, step, broad), BF16)] * 2
        + [pltpu.VMEM((tall, broad), F32), pltpu.SemaphoreType.DMA((2,))],
        compiler_params=pltpu.CompilerParams(vmem_limit_bytes=12 << 20),
        cost_estimate=cost(2),
    )(total, held_left, held_high, held_low, last_a, last_s, *far_b)


def solution(mesh):
    placed = (P("row", "col"), P("row", "col"))
    return jax.shard_map(product, mesh=mesh, in_specs=placed, out_specs=P("row", "col"), check_vma=False)
```

```python
import jax
import jax.numpy as jnp
from jax import lax
from jax.experimental import pallas as pl
from jax.experimental.pallas import tpu as pltpu
from jax.sharding import PartitionSpec as P


BOTH = ("row", "col")
Y, XH, XL, Z, CORE = 4, 2, 2, 4, 2
F32, BF16 = jnp.float32, jnp.bfloat16


def pairs(move):
    listed = []
    for y in range(Y):
        for x in range(XH * XL):
            for z in range(Z):
                for core in range(CORE):
                    y2, x2, z2, core2 = move(y, x, z, core)
                    y2, x2, z2 = y2 % Y, x2 % (XH * XL), z2 % Z
                    source = ((y * XH + x // XL) * XL + x % XL) * Z + z
                    target = ((y2 * XH + x2 // XL) * XL + x2 % XL) * Z + z2
                    listed.append((source * CORE + core, target * CORE + core2))
    return listed


MOVES = {
    "z+": pairs(lambda y, x, z, c: (y, x, z + 1, 1 - c)),
    "z-": pairs(lambda y, x, z, c: (y, x, z - 1, 1 - c)),
    "y+": pairs(lambda y, x, z, c: (y + 1, x, z, c)),
    "y-": pairs(lambda y, x, z, c: (y - 1, x, z, c)),
    "lo": pairs(lambda y, x, z, c: (y, x ^ 1, z, 1 - c)),
    "hi": pairs(lambda y, x, z, c: (y, x ^ 2, z, c)),
    "core": pairs(lambda y, x, z, c: (y, x, z, 1 - c)),
}


def send(array, move):
    return lax.ppermute(array, BOTH, MOVES[move])


def cut(array, top, rows):
    return array[top : top + rows]


def cat(*arrays):
    return jnp.concatenate(arrays)


def place():
    row, col = lax.axis_index("row"), lax.axis_index("col")
    y, xh = row >> 1, row & 1
    xl, z, core = col >> 3, (col >> 1) & 3, col & 1
    left = lambda other, turn: ((xl ^ other) * Z) + ((z + turn) & 3)
    right = lambda other, turn: (((y + turn) & 3) * XH) + (xh ^ other)
    return left, right, core


def split(value):
    high = value.astype(BF16)
    return high, (value - high.astype(F32)).astype(BF16)


def mul(*terms):
    lefts, rights = [], []
    for left, high, low in terms:
        left_high, left_low = split(left)
        lefts += [left_high, left_low, left_high]
        rights += [high, high, low]
    return jnp.dot(jnp.concatenate(lefts, axis=1), jnp.concatenate(rights), preferred_element_type=F32)


LEFTS = ((0, 0), (1, 0), (0, 3), (0, 1), (0, 2), (1, 3), (1, 1))
ROWS, FAR, UPPER = 64, 256, 320
RIGHTS = (
    (0, 0, 0), (0, 3, 0), (0, 1, 0), (0, 2, 0), (0, 2, FAR), (1, 0, 0), (1, 0, UPPER),
    (1, 3, 0), (1, 1, 0), (1, 3, UPPER), (1, 1, UPPER),
)
SOON, HELD = 4, 7


def store_right(refs, places, right_of, high, low):
    step = high.shape[1]
    for ref, (other, turn, top) in zip(refs, places):
        for part in range(0, ref.shape[0], ROWS):
            at, rows = right_of(other, turn) * 2 + (top + part) // step, pl.ds((top + part) % step, ROWS)
            high[at, rows], low[at, rows] = split(ref[part : part + ROWS])


def add(total, mine, theirs, place_of, left_of, core, high, low):
    other, turn = place_of
    tile = left_of(other, turn)
    rows, step = mine.shape[0], high.shape[1]
    side = (core + other + turn) & 1
    at, beside = tile * 2 + side, tile * 2 + 1 - side
    for block in range(rows // step):
        rows_in = pl.ds(block * step, step)
        total[rows_in] += mul((mine[rows_in], high[at], low[at]), (theirs[rows_in], high[beside], low[beside]))


def is_soon(tile, right_of):
    return ((tile & 1) == (right_of(0, 0) & 1)) | (tile == right_of(1, 0))


def parts(ref, count):
    rows = ref.shape[0] // count
    return tuple(ref.at[pl.ds(index * rows, rows)] for index in range(count))


def soon_kernel(*refs):
    mine, rights = refs[:SOON], refs[SOON + 2 : SOON + 2 + HELD]
    theirs = (refs[SOON], *parts(refs[SOON + 1], SOON - 1))
    total, high, low = refs[SOON + 2 + HELD :]
    left_of, right_of, core = place()
    store_right(rights, RIGHTS[:HELD], right_of, high, low)
    total[...] = jnp.zeros_like(total)
    for mine_ref, their_ref, where in zip(mine, theirs, LEFTS):

        @pl.when(is_soon(left_of(*where), right_of))
        def _():
            add(total, mine_ref, their_ref, where, left_of, core, high, low)


def main_kernel(*refs):
    count, late = len(LEFTS), len(RIGHTS) - HELD
    mine, rights = refs[:count], refs[count + 4 : count + 4 + late]
    own, one, far, two = refs[count : count + 4]
    theirs = (own, *parts(one, SOON - 1), far, *parts(two, 2))
    _, _, _, total, high, low, held_left, held_high, held_low = refs[count + 4 + late :]
    left_of, right_of, core = place()
    last = right_of(1, 2)
    spare = left_of(1, 2)

    store_right(rights, RIGHTS[HELD:], right_of, high, low)
    for part in range(2):
        high[last * 2 + part] = jnp.zeros(high.shape[1:], BF16)
        low[last * 2 + part] = jnp.zeros(low.shape[1:], BF16)

    @pl.when(last == spare)
    def _():
        held_left[...] = jnp.zeros_like(held_left)

    for part in range(2):
        held_high[part] = high[spare * 2 + part]
        held_low[part] = low[spare * 2 + part]

    for index, (mine_ref, their_ref, where) in enumerate(zip(mine, theirs, LEFTS)):
        other, turn = where
        tile = left_of(other, turn)
        open_still = tile != last
        if index < SOON:
            open_still &= jnp.logical_not(is_soon(tile, right_of))

        @pl.when(open_still)
        def _():
            add(total, mine_ref, their_ref, where, left_of, core, high, low)

        @pl.when(tile == last)
        def _():
            side = (core + other + turn) & 1
            held_left[side] = mine_ref[...]
            held_left[1 - side] = their_ref[...]


def last_kernel(total, held_left, held_high, held_low, mine, theirs, b0, b1, out, high, low, done, sems):
    left_of, right_of, core = place()
    last = right_of(1, 2)
    spare = left_of(1, 2)
    step = high.shape[1]
    for ref, top in ((b0, 0), (b1, UPPER)):
        for part in range(0, ref.shape[0], ROWS):
            at, rows = (top + part) // step, pl.ds((top + part) % step, ROWS)
            high[at, rows], low[at, rows] = split(ref[part : part + ROWS])

    @pl.when(last == spare)
    def _():
        held_high[...] = high[...]
        held_low[...] = low[...]

    side = 1 - core
    copies = []
    for block in range(mine.shape[0] // step):
        rows = pl.ds(block * step, step)
        done[rows] = total[rows] + mul(
            (mine[rows], held_high[side], held_low[side]),
            (theirs[rows], held_high[1 - side], held_low[1 - side]),
            (held_left[0, rows], high[0], low[0]),
            (held_left[1, rows], high[1], low[1]),
        )
        copies.append(pltpu.make_async_copy(done.at[rows], out.at[rows], sems.at[block]))
        copies[-1].start()
    for copy in copies:
        copy.wait()


def product(a, b):
    tall, wide = a.shape
    deep, broad = b.shape
    half, hill = deep // 2, tall // 2
    inside = pl.BlockSpec(memory_space=pltpu.VMEM)

    a_lo = send(a, "lo")
    a_p, a_m = send(a, "z+"), send(a, "z-")
    b_p, b_m = send(b, "y+"), send(b, "y-")
    b_hi = [send(cut(b, 0, UPPER), "hi"), send(cut(b, UPPER, deep - UPPER), "hi")]
    al_p, al_m = send(a_lo, "z+"), send(a_lo, "z-")
    a_pp = send(cut(a_p, 0, hill), "z+")
    a_mm = send(cut(a_m, hill, hill), "z-")
    b_pp = send(cut(b_p, 0, FAR), "y+")
    b_mm = send(cut(b_m, FAR, deep - FAR), "y-")
    bh_p = [send(b_hi[0], "y+"), send(b_hi[1], "y+")]
    bh_m = [send(b_hi[0], "y-"), send(b_hi[1], "y-")]
    al_pp = send(cut(al_p, 0, hill), "z+")
    al_mm = send(cut(al_m, hill, hill), "z-")
    far_b = send(bh_p[0], "y+"), send(bh_m[1], "y-")

    a_far = cat(a_pp, a_mm)
    lefts = (a, a_lo, a_p, a_m, a_far, al_p, al_m)
    own = send(a, "core")
    one = send(cat(a_lo, a_p, a_m), "core")
    two = send(cat(al_p, al_m), "core")
    far = send(a_far, "core")
    rights = (b, b_p, b_m, b_pp, b_mm, b_hi[0], b_hi[1], bh_p[0], bh_m[0], bh_p[1], bh_m[1])
    step = half
    flops = 6 * tall * deep * XL * Z * broad
    shape = jax.ShapeDtypeStruct
    whole, panel = shape((tall, broad), F32), shape((XL * Z * 2, step, broad), BF16)

    def cost(part):
        return pl.CostEstimate(flops=flops * part // 8, bytes_accessed=part << 20, transcendentals=0)

    soon = (*lefts[:SOON], own, one, *rights[:HELD])
    total, high, low = pl.pallas_call(
        soon_kernel,
        out_shape=(whole, panel, panel),
        in_specs=[inside] * len(soon),
        out_specs=(inside,) * 3,
        compiler_params=pltpu.CompilerParams(vmem_limit_bytes=16 << 20),
        cost_estimate=cost(2),
    )(*soon)
    later = (*lefts, own, one, far, two, *rights[HELD:])
    total, _, _, held_left, held_high, held_low = pl.pallas_call(
        main_kernel,
        out_shape=(
            whole, panel, panel,
            shape((2, tall, wide), F32),
            shape((2, step, broad), BF16),
            shape((2, step, broad), BF16),
        ),
        in_specs=[inside] * (len(later) + 3),
        out_specs=(inside,) * 6,
        input_output_aliases={len(later) + index: index for index in range(3)},
        compiler_params=pltpu.CompilerParams(vmem_limit_bytes=16 << 20),
        cost_estimate=cost(5),
    )(*later, total, high, low)

    last_a = cat(al_pp, al_mm)
    last_s = send(last_a, "core")
    return pl.pallas_call(
        last_kernel,
        out_shape=jax.ShapeDtypeStruct((tall, broad), F32),
        in_specs=[inside] * 8,
        out_specs=pl.BlockSpec(memory_space=pl.ANY),
        scratch_shapes=[pltpu.VMEM((2, step, broad), BF16)] * 2
        + [pltpu.VMEM((tall, broad), F32), pltpu.SemaphoreType.DMA((2,))],
        compiler_params=pltpu.CompilerParams(vmem_limit_bytes=12 << 20),
        cost_estimate=cost(2),
    )(total, held_left, held_high, held_low, last_a, last_s, *far_b)


def solution(mesh):
    placed = (P("row", "col"), P("row", "col"))
    return jax.shard_map(product, mesh=mesh, in_specs=placed, out_specs=P("row", "col"), check_vma=False)
```
